32 devices in a mesh: ta: 4 (over y, x), gz: 2 (over core), gy: 4 (over z).
Axes of the slice: x: 2, y: 2, z: 4, core: 2. Of those that a mesh axis runs over, the one named last changes fastest.
Arguments:
- source: float32 [2, 3, 8, 8, 512], P(None, None, 'ta', 'gz', 'gy'), may hold values from -40 to 40
- fat_links: bfloat16 [2, 4, 2, 3, 3, 8, 8, 512], P(None, None, None, None, None, 'ta', 'gz', 'gy'), may hold values from -1.25 to 1.25
- long_links: bfloat16 [2, 4, 2, 3, 3, 8, 8, 512], P(None, None, None, None, None, 'ta', 'gz', 'gy'), may hold values from -0.625 to 0.625
Outputs:
- solution: float32 [2, 3, 8, 8, 512], P(None, None, 'ta', 'gz', 'gy')
- true_residual: float32 [2, 3, 8, 8, 512], P(None, None, 'ta', 'gz', 'gy')
The draws below stay inside these ranges and needn't reach their ends.
All inputs are finite; a program needn't handle non-finite values.
Results may differ from the reference program's by a relative error of at most 0.00085.
Values may be sent and summed in bfloat16 or wider, within the bound.
No kernel may reach another device: no remote copies, remote signals or barrier semaphores. Data moves between devices by JAX's collectives and lax.ppermute only.
A program may use at most 128 MiB of HBM per device.

```python
import jax
import jax.numpy as jnp

NX = 32
ITERS = 8
NTH = 8
NZ = 8
NYX = 512


def draw_source(key, part):
    base = jax.random.normal(key, (2, 3, NTH, NZ, NYX), jnp.float32)
    base = jnp.clip(base, -3.5, 3.5)
    rows = jnp.arange(NTH, dtype=jnp.float32) / max(NTH - 1, 1)
    scale = 3.0 ** rows
    value = base * scale[None, None, :, None, None]
    return jnp.clip(value, -40.0, 40.0)


def steps_of(own_key, shape, cuts, least, top_value):
    def one(dim, parts):
        draws = jax.random.uniform(jax.random.fold_in(jax.random.fold_in(own_key, 6), dim), (parts,), jnp.float32, least / len(cuts), top_value / len(cuts))
        return jnp.repeat(jnp.exp(draws), shape[dim] // parts).reshape((-1,) + (1,) * (len(shape) - dim - 1))

    loudness = one(*cuts[0])
    for cut in cuts[1:]:
        loudness = loudness * one(*cut)
    return loudness


def gaussian(rng, dims, spread, bound, pieces=(), kind=jnp.bfloat16):
    entries = spread * jax.random.normal(rng, dims, jnp.float32)
    if pieces:
        entries = entries * steps_of(rng, dims, pieces, -0.22, 0.18)
    return jnp.clip(entries, -bound, bound).astype(kind)


def setup_inputs(seed: int = 0) -> dict:
    seeds = jax.random.split(jax.random.key(seed), 4)
    source = draw_source(jax.random.fold_in(seeds[3], 71), 0)
    fat_links = gaussian(seeds[1], (2, 4, 2, 3, 3, NTH, NZ, NYX), 0.2, 1.25, ((5, 4), (6, 2), (7, 4)))
    long_links = gaussian(seeds[2], (2, 4, 2, 3, 3, NTH, NZ, NYX), 0.1, 0.625, ((5, 4), (6, 2), (7, 4)))
    return dict(source=source, fat_links=fat_links, long_links=long_links)


mass_squared = 0.1


def mat_vec(link, vector):
    real_a, imag_a = link[0], link[1]
    real_v, imag_v = vector[0], vector[1]
    real_o = jnp.sum(real_a * real_v[None] - imag_a * imag_v[None], axis=1)
    imag_o = jnp.sum(real_a * imag_v[None] + imag_a * real_v[None], axis=1)
    return jnp.stack([real_o, imag_o])


def adj_vec(link, vector):
    real_a, imag_a = link[0], link[1]
    real_v, imag_v = vector[0], vector[1]
    real_o = jnp.sum(real_a * real_v[:, None] + imag_a * imag_v[:, None], axis=0)
    imag_o = jnp.sum(real_a * imag_v[:, None] - imag_a * real_v[:, None], axis=0)
    return jnp.stack([real_o, imag_o])


def parity_mask(z_len, yx_len):
    zeds = jnp.arange(z_len, dtype=jnp.int32)[:, None]
    cells = jnp.arange(yx_len, dtype=jnp.int32)[None, :]
    return ((zeds + cells // NX + cells % NX) % 2) == 1


def roll_x(field, shift):
    shape = field.shape
    folded = field.reshape(shape[:-1] + (shape[-1] // NX, NX))
    return jnp.roll(folded, shift, axis=-1).reshape(shape)


def reference(source, fat_links, long_links):
    mask = parity_mask(source.shape[3], source.shape[4])

    def dslash(src, dst, srcp):
        select = mask if dst == 0 else jnp.logical_not(mask)
        total = jnp.zeros(src.shape, jnp.float32)
        for mu in range(4):
            fat_dst = fat_links[dst, mu].astype(jnp.float32)
            long_dst = long_links[dst, mu].astype(jnp.float32)
            back1 = adj_vec(fat_links[srcp, mu].astype(jnp.float32), src)
            back3 = adj_vec(long_links[srcp, mu].astype(jnp.float32), src)
            if mu == 0:
                one = jnp.where(select, jnp.roll(src, -1, 2), src)
                three = jnp.where(select, jnp.roll(src, -2, 2), jnp.roll(src, -1, 2))
                low1 = jnp.where(select, back1, jnp.roll(back1, 1, 2))
                low3 = jnp.where(select, jnp.roll(back3, 1, 2), jnp.roll(back3, 2, 2))
            elif mu == 1:
                one = jnp.roll(src, -1, 3)
                three = jnp.roll(src, -3, 3)
                low1 = jnp.roll(back1, 1, 3)
                low3 = jnp.roll(back3, 3, 3)
            elif mu == 2:
                one = jnp.roll(src, -NX, 4)
                three = jnp.roll(src, -3 * NX, 4)
                low1 = jnp.roll(back1, NX, 4)
                low3 = jnp.roll(back3, 3 * NX, 4)
            else:
                one = roll_x(src, -1)
                three = roll_x(src, -3)
                low1 = roll_x(back1, 1)
                low3 = roll_x(back3, 3)
            total = total + (mat_vec(fat_dst, one) + mat_vec(long_dst, three) - low1 - low3)
        return total

    def normal_op(vector):
        return mass_squared * vector - dslash(dslash(vector, 1, 0), 0, 1)

    solution = jnp.zeros(source.shape, jnp.float32)
    residual = source
    direction = source
    norm_now = jnp.sum(residual * residual)
    for step in range(ITERS):
        image = normal_op(direction)
        alpha = norm_now / jnp.sum(direction * image)
        solution = solution + alpha * direction
        residual = residual - alpha * image
        norm_next = jnp.sum(residual * residual)
        direction = residual + (norm_next / norm_now) * direction
        norm_now = norm_next
    return solution, source - normal_op(solution)
```

```python
import jax
import jax.numpy as jnp
from jax import lax
from jax.experimental import pallas as pl
from jax.experimental.pallas import tpu as pltpu
from jax.sharding import PartitionSpec as P

NX = 32
ITERS = 8
STEPS = 2

mass_squared = 0.1
SCALE = 1.0 / 16.0

VMEM = pl.BlockSpec(memory_space=pltpu.VMEM)
PARAMS = pltpu.CompilerParams(vmem_limit_bytes=4 * 2**20)
AXES = ("ta", "gz", "gy")


def on_core(body, outs, *args):
    return pl.pallas_call(
        body,
        out_shape=tuple(jax.ShapeDtypeStruct(shape, jnp.float32) for shape in outs),
        in_specs=[VMEM] * len(args),
        out_specs=tuple(VMEM for _ in outs),
        compiler_params=PARAMS,
    )(*args)


def passed_along(shard, axis, by):
    size = lax.axis_size(axis)
    return lax.ppermute(shard, axis, [(i, (i + by) % size) for i in range(size)])


def rolled(tile, shift, axis):
    shift = shift % tile.shape[axis]
    return pltpu.roll(tile, shift, axis) if shift else tile


class Shifts:
    def __init__(self, rows, depth, width):
        self.rows, self.depth, self.width = (rows, depth, width)
        self.shape = (rows * depth, width)
        sub = lax.broadcasted_iota(jnp.int32, self.shape, 0)
        self.lane = lax.broadcasted_iota(jnp.int32, self.shape, 1)
        self.row = sub // depth
        self.plane = sub % depth
        self.x = self.lane % NX
        self.odd = (self.plane + self.lane // NX + self.x) % 2 == 1

    def select(self, dst):
        return self.odd if dst == 0 else jnp.logical_not(self.odd)

    def t_rows(self, own, other, by):
        if by == 0:
            return own
        near = self.row >= by if by > 0 else self.row < self.rows + by
        return rolled(jnp.where(near, own, other), -by * self.depth, 0)

    def t(self, own, other, by, dst):
        sel = self.select(dst)
        half = {1: (1, 0), 3: (2, 1), -1: (0, -1), -3: (-1, -2)}[by]
        return jnp.where(sel, self.t_rows(own, other, half[0]), self.t_rows(own, other, half[1]))

    def z(self, own, other, by):
        near = self.plane < self.depth - by if by > 0 else self.plane >= -by
        wrap = self.depth - by if by > 0 else -self.depth - by
        return jnp.where(near, rolled(own, -by, 0), rolled(other, wrap, 0))

    def y(self, own, other, by):
        lanes = by * NX
        near = self.lane >= lanes if by > 0 else self.lane < self.width + lanes
        return rolled(jnp.where(near, own, other), -lanes, 1)

    def x_(self, own, by):
        near = self.x < NX - by if by > 0 else self.x >= -by
        wrap = NX - by if by > 0 else -NX - by
        return jnp.where(near, rolled(own, -by, 1), rolled(own, wrap, 1))

    def hop(self, own, other, mu, by, dst):
        if mu == 0:
            return self.t(own, other, by, dst)
        if mu == 1:
            return self.z(own, other, by)
        if mu == 2:
            return self.y(own, other, by)
        return self.x_(own, by)


HOPS = tuple((mu, by) for mu in range(4) for by in (1, 3, -1, -3))


def link_tables(fat, long, near, dims):
    rows, depth, width = dims
    tile = (rows * depth, width)

    def body(fat_ref, long_ref, t_ref, z_ref, y_ref, out0, out1):
        shifts = Shifts(rows, depth, width)
        lows = (t_ref, z_ref, y_ref)
        for dst, out in ((0, out0), (1, out1)):

            def entry(i, carry):
                flip = 3 * (i % 3) + i // 3
                for k, (mu, by) in enumerate(HOPS):
                    kind = 0 if abs(by) == 1 else 1
                    ref = (fat_ref, long_ref)[kind]
                    for part in range(2):
                        if by > 0:
                            value = ref[dst, mu, 9 * part + i].astype(jnp.float32)
                            out[18 * k + 9 * part + i] = value
                        else:
                            own = ref[1 - dst, mu, 9 * part + i].astype(jnp.float32)
                            other = own
                            if mu < 3:
                                other = lows[mu][kind, 1 - dst, 9 * part + i].astype(jnp.float32)
                            value = shifts.hop(own, other, mu, by, dst)
                            out[18 * k + 9 * part + flip] = value if part else -value
                return carry

            lax.fori_loop(0, 9, entry, 0)

    return on_core(body, [(18 * len(HOPS),) + tile] * 2, fat, long, *near)


def hopping_sum(shifts, field, near, table, dst):
    total = [None] * 6
    for k, (mu, by) in enumerate(HOPS):
        ref = near[2 * mu + (0 if by > 0 else 1)] if mu < 3 else None
        hopped = [
            shifts.hop(field[c], ref[c] if mu < 3 else None, mu, by, dst) for c in range(6)
        ]
        for a in range(3):
            re = im = None
            for b in range(3):
                lre = table[18 * k + 3 * a + b]
                lim = table[18 * k + 9 + 3 * a + b]
                vre, vim = (hopped[b], hopped[3 + b])
                one, two = (lre * vre - lim * vim, lre * vim + lim * vre)
                re = one if re is None else re + one
                im = two if im is None else im + two
            total[a] = re if total[a] is None else total[a] + re
            total[3 + a] = im if total[3 + a] is None else total[3 + a] + im
    return total


def neighbours(field):
    zp = passed_along(field, "gz", -1)
    zm = zp if lax.axis_size("gz") == 2 else passed_along(field, "gz", 1)
    return (
        passed_along(field, "ta", -1),
        passed_along(field, "ta", 1),
        zp,
        zm,
        passed_along(field, "gy", -1),
        passed_along(field, "gy", 1),
    )


def odd_from_even(field, table, dims):
    def body(field_ref, tp, tm, zp, zm, yp, ym, table_ref, out):
        shifts = Shifts(*dims)
        for c, value in enumerate(
            hopping_sum(shifts, field_ref, (tp, tm, zp, zm, yp, ym), table_ref, 1)
        ):
            out[c] = value

    return on_core(body, [field.shape], field, *neighbours(field), table)[0]


def even_from_odd(field, start, table, dims, scale, base=None):
    def body(field_ref, tp, tm, zp, zm, yp, ym, table_ref, start_ref, *rest):
        shifts = Shifts(*dims)
        out = rest[-1]
        for c, value in enumerate(
            hopping_sum(shifts, field_ref, (tp, tm, zp, zm, yp, ym), table_ref, 0)
        ):
            image = scale * (mass_squared * start_ref[c] - value)
            out[c] = image if base is None else rest[0][c] - image

    extra = () if base is None else (base,)
    return on_core(body, [field.shape], field, *neighbours(field), table, start, *extra)[0]


def pairs_of(first):
    live = range(3 if first else 0, 6)
    return tuple((i, j) for i in live for j in live if i <= j)


def gram_parts(basis, copies):
    shape = basis[0].shape
    first = len(basis) == 3
    pairs = pairs_of(first)
    skip = 3 if first else 0

    def body(*refs):
        out = refs[-1]
        lane = lax.broadcasted_iota(jnp.int32, (8, 128), 1)
        row = lax.broadcasted_iota(jnp.int32, (8, 128), 0)
        packed = jnp.zeros((8, 128), jnp.float32)
        for n, (i, j) in enumerate(pairs):
            left, right = (refs[i - skip], refs[j - skip])
            tile = left[0] * right[0]
            for c in range(1, shape[0]):
                tile = tile + left[c] * right[c]
            value = jnp.sum(jnp.sum(tile, axis=0, keepdims=True), axis=1, keepdims=True)
            here = jnp.logical_and(row == n % 8, lane == n // 8)
            packed = jnp.where(here, value, packed)
        for k in range(copies):
            out[k] = packed

    return on_core(body, [(copies, 8, 128)], *basis)[0]


def block_update(sums, state, basis, solution):
    shape = basis[0].shape
    tile = shape[1:]
    first = state is None
    live = range(3 if first else 0, 6)
    before = () if first else (state, solution)

    def body(sums_ref, *refs):
        refs = list(refs)
        vectors = {i: refs.pop(0) for i in live}
        if not first:
            state_ref, solution_ref = (refs.pop(0), refs.pop(0))
            norm_before, alpha_before = (state_ref[0], state_ref[1])
        state_out, x_out, r_out, p_out, q_out, w_out = refs
        total = sums_ref[0]
        for k in range(1, sums_ref.shape[0]):
            total = total + sums_ref[k]
        gram = {}
        for n, (i, j) in enumerate(pairs_of(first)):
            value = jnp.broadcast_to(total[n % 8 : n % 8 + 1, n // 8 : n // 8 + 1], tile)
            gram[i, j] = gram[j, i] = value

        def add(a, b):
            return b if a is None else a if b is None else a + b

        def times(s, vec):
            return {i: s * v for i, v in vec.items()}

        def plus(u, v):
            return {i: add(u.get(i), v.get(i)) for i in sorted(set(u) | set(v))}

        def dot(u, v):
            out = None
            for i, a in u.items():
                part = None
                for j, b in v.items():
                    part = add(part, gram[i, j] * b)
                out = add(out, a * part)
            return out

        def applied(u):
            out = {}
            for i, a in u.items():
                if i == 0:
                    out = plus(out, {1: a})
                elif i == 1:
                    share = a / alpha_before
                    out = plus(out, {2: share, 4: share * (-1.0 / SCALE)})
                elif i in (3, 4):
                    out = plus(out, {i + 1: a * (1.0 / SCALE)})
            return out

        residual = {3: jnp.ones(tile, jnp.float32)}
        norm = gram[3, 3]
        direction = residual if first else {0: norm / norm_before, **residual}
        gain = {}
        for step in range(STEPS):
            if step:
                norm_next = dot(residual, residual)
                direction = plus(residual, times(norm_next / norm, direction))
                norm = norm_next
            image = applied(direction)
            alpha = norm / dot(direction, image)
            gain = plus(gain, times(alpha, direction))
            last = residual
            residual = plus(residual, times(-alpha, image))
        state_out[0] = norm
        state_out[1] = alpha
        shown = ((r_out, residual), (p_out, direction), (q_out, image), (w_out, applied(last)))
        for c in range(shape[0]):
            values = {i: vectors[i][c] for i in live}
            grown = sum(s * values[i] for i, s in gain.items())
            x_out[c] = grown if first else solution_ref[c] + grown
            for out, coefs in shown:
                out[c] = sum(s * values[i] for i, s in coefs.items())

    outs = [(2,) + tile] + [shape] * 5
    return on_core(body, outs, sums, *basis, *before)


def per_device(source, fat_links, long_links):
    rows, depth, width = source.shape[2:]
    dims = (rows, depth, width)
    tile = (rows * depth, width)
    field = source.reshape((6,) + tile)
    fat = fat_links.reshape((2, 4, 18) + tile)
    long = long_links.reshape((2, 4, 18) + tile)
    near = [
        passed_along(jnp.stack([fat[:, mu], long[:, mu]]), axis, 1)
        for mu, axis in enumerate(AXES)
    ]
    even_table, odd_table = link_tables(fat, long, near, dims)

    devices = 1
    for axis in AXES:
        devices *= lax.axis_size(axis)

    def powers(vector):
        odd = odd_from_even(vector, odd_table, dims)
        return even_from_odd(odd, vector, even_table, dims, SCALE)

    solution = state = None
    residual = field
    back = ()
    for _ in range(ITERS // STEPS):
        one = powers(residual)
        two = powers(one)
        basis = back + (residual, one, two)
        parts = gram_parts(basis, devices)
        sums = lax.all_to_all(parts, AXES, 0, 0, tiled=True)
        state, solution, residual, *back = block_update(sums, state, basis, solution)
        back = tuple(back)
    odd = odd_from_even(solution, odd_table, dims)
    true = even_from_odd(odd, solution, even_table, dims, 1.0, base=field)
    return (solution.reshape(source.shape), true.reshape(source.shape))


def solution(mesh):
    in_specs = (
        P(None, None, "ta", "gz", "gy"),
        P(None, None, None, None, None, "ta", "gz", "gy"),
        P(None, None, None, None, None, "ta", "gz", "gy"),
    )
    out_specs = (P(None, None, "ta", "gz", "gy"), P(None, None, "ta", "gz", "gy"))
    return jax.shard_map(
        per_device, mesh=mesh, in_specs=in_specs, out_specs=out_specs, check_vma=False
    )
```

```python
import jax
import jax.numpy as jnp
from jax import lax
from jax.experimental import pallas as pl
from jax.experimental.pallas import tpu as pltpu
from jax.sharding import PartitionSpec as P

NX = 32
ITERS = 8
FIRST = 2

mass_squared = 0.1
SCALE = 1.0 / 16.0

VMEM = pl.BlockSpec(memory_space=pltpu.VMEM)
PARAMS = pltpu.CompilerParams(vmem_limit_bytes=4 * 2**20)
AXES = ("ta", "gz", "gy")


def on_core(body, outs, *args):
    return pl.pallas_call(
        body,
        out_shape=tuple(jax.ShapeDtypeStruct(shape, jnp.float32) for shape in outs),
        in_specs=[VMEM] * len(args),
        out_specs=tuple(VMEM for _ in outs),
        compiler_params=PARAMS,
    )(*args)


def passed_along(shard, axis, by):
    size = lax.axis_size(axis)
    return lax.ppermute(shard, axis, [(i, (i + by) % size) for i in range(size)])


def swapped(shard, axis, odd):
    size = lax.axis_size(axis)
    assert size % 2 == 0
    ahead = [(i, (i + 1) % size) for i in range(odd, size, 2)]
    return lax.ppermute(shard, axis, ahead + [(j, i) for i, j in ahead])


def rolled(tile, shift, axis):
    shift = shift % tile.shape[axis]
    return pltpu.roll(tile, shift, axis) if shift else tile


class Shifts:
    def __init__(self, rows, depth, width):
        self.rows, self.depth, self.width = (rows, depth, width)
        self.shape = (rows * depth, width)
        sub = lax.broadcasted_iota(jnp.int32, self.shape, 0)
        self.lane = lax.broadcasted_iota(jnp.int32, self.shape, 1)
        self.row = sub // depth
        self.plane = sub % depth
        self.x = self.lane % NX
        self.odd = (self.plane + self.lane // NX + self.x) % 2 == 1

    def select(self, dst):
        return self.odd if dst == 0 else jnp.logical_not(self.odd)

    def t_rows(self, own, other, by):
        if by == 0:
            return own
        near = self.row >= by if by > 0 else self.row < self.rows + by
        return rolled(jnp.where(near, own, other), -by * self.depth, 0)

    def t(self, own, other, by, dst):
        sel = self.select(dst)
        half = {1: (1, 0), 3: (2, 1), -1: (0, -1), -3: (-1, -2)}[by]
        return jnp.where(sel, self.t_rows(own, other, half[0]), self.t_rows(own, other, half[1]))

    def z(self, own, other, by):
        near = self.plane < self.depth - by if by > 0 else self.plane >= -by
        wrap = self.depth - by if by > 0 else -self.depth - by
        return jnp.where(near, rolled(own, -by, 0), rolled(other, wrap, 0))

    def y(self, own, other, by):
        lanes = by * NX
        near = self.lane >= lanes if by > 0 else self.lane < self.width + lanes
        return rolled(jnp.where(near, own, other), -lanes, 1)

    def x_(self, own, by):
        near = self.x < NX - by if by > 0 else self.x >= -by
        wrap = NX - by if by > 0 else -NX - by
        return jnp.where(near, rolled(own, -by, 1), rolled(own, wrap, 1))

    def hop(self, own, other, mu, by, dst):
        if mu == 0:
            return self.t(own, other, by, dst)
        if mu == 1:
            return self.z(own, other, by)
        if mu == 2:
            return self.y(own, other, by)
        return self.x_(own, by)


HOPS = tuple((mu, by) for mu in range(4) for by in (1, 3, -1, -3))


def link_table(fat, long, near, dims, dst):
    rows, depth, width = dims
    tile = (rows * depth, width)

    def body(fat_ref, long_ref, t_ref, z_ref, y_ref, out):
        shifts = Shifts(rows, depth, width)
        lows = (t_ref, z_ref, y_ref)

        def entry(i, carry):
            flip = 3 * (i % 3) + i // 3
            for k, (mu, by) in enumerate(HOPS):
                kind = 0 if abs(by) == 1 else 1
                ref = (fat_ref, long_ref)[kind]
                for part in range(2):
                    if by > 0:
                        value = ref[dst, mu, 9 * part + i].astype(jnp.float32)
                        out[18 * k + 9 * part + i] = value
                    else:
                        own = ref[1 - dst, mu, 9 * part + i].astype(jnp.float32)
                        other = own
                        if mu < 3:
                            other = lows[mu][kind, 1 - dst, 9 * part + i].astype(jnp.float32)
                        value = shifts.hop(own, other, mu, by, dst)
                        out[18 * k + 9 * part + flip] = value if part else -value
            return carry

        lax.fori_loop(0, 9, entry, 0)

    return on_core(body, [(18 * len(HOPS),) + tile], fat, long, *near)[0]


def hopping_sum(shifts, field, near, table, dst):
    flags = near[-1]
    total = [None] * 6
    for mu in range(4):
        ahead = behind = [None] * 6
        if mu < 3:
            one, two = (near[2 * mu], near[2 * mu + 1])
            if one is two:
                ahead = behind = [one[c] for c in range(6)]
            else:
                even = flags[mu] > 0.5
                pairs = [(one[c], two[c]) for c in range(6)]
                ahead = [jnp.where(even, u, v) for u, v in pairs]
                behind = [jnp.where(even, v, u) for u, v in pairs]
        for k, (axis, by) in enumerate(HOPS):
            if axis != mu:
                continue
            other = ahead if by > 0 else behind
            hopped = [shifts.hop(field[c], other[c], mu, by, dst) for c in range(6)]
            for a in range(3):
                re = im = None
                for b in range(3):
                    lre = table[18 * k + 3 * a + b]
                    lim = table[18 * k + 9 + 3 * a + b]
                    vre, vim = (hopped[b], hopped[3 + b])
                    x, y = (lre * vre - lim * vim, lre * vim + lim * vre)
                    re = x if re is None else re + x
                    im = y if im is None else im + y
                total[a] = re if total[a] is None else total[a] + re
                total[3 + a] = im if total[3 + a] is None else total[3 + a] + im
    return total


def axis_sizes():
    return tuple(lax.axis_size(axis) for axis in AXES)


def swaps_of(sizes):
    return tuple(
        (mu, odd) for odd in (1, 0) for mu in (2, 0, 1) if odd == 0 or sizes[mu] > 2
    )


def neighbours(field):
    return tuple(swapped(field, AXES[mu], odd) for mu, odd in swaps_of(axis_sizes()))


def spread(refs, sizes):
    keys = swaps_of(sizes)
    got = dict(zip(keys, refs))
    near = [got.get((mu, odd), got[mu, 0]) for mu in range(3) for odd in (0, 1)]
    return near, list(refs[len(keys) :])


def odd_from_even(field, table, flags, dims):
    sizes = axis_sizes()

    def body(field_ref, table_ref, flags_ref, *refs):
        near, (out,) = spread(refs, sizes)
        shifts = Shifts(*dims)
        for c, value in enumerate(hopping_sum(shifts, field_ref, near + [flags_ref], table_ref, 1)):
            out[c] = value

    return on_core(body, [field.shape], field, table, flags, *neighbours(field))[0]


def even_from_odd(field, start, table, flags, dims, finish, *extra):
    sizes = axis_sizes()

    def body(field_ref, start_ref, table_ref, flags_ref, *refs):
        near, rest = spread(refs, sizes)
        more, out = (rest[:-1], rest[-1])
        shifts = Shifts(*dims)
        for c, value in enumerate(hopping_sum(shifts, field_ref, near + [flags_ref], table_ref, 0)):
            out[c] = finish(c, mass_squared * start_ref[c] - value, start_ref, more)

    near = neighbours(field)
    return on_core(body, [field.shape], field, start, table, flags, *near, *extra)[0]


def pairs_of(count):
    return tuple((i, j) for i in range(count) for j in range(i, count))


def gram_parts(basis, copies):
    parts, width = (basis[0].shape[0], 128)

    def body(*refs):
        out = refs[-1]
        lane = lax.broadcasted_iota(jnp.int32, (8, width), 1)
        row = lax.broadcasted_iota(jnp.int32, (8, width), 0)
        packed = jnp.zeros((8, width), jnp.float32)
        for n, (i, j) in enumerate(pairs_of(len(basis))):
            tile = refs[i][0] * refs[j][0]
            for c in range(1, parts):
                tile = tile + refs[i][c] * refs[j][c]
            value = jnp.sum(jnp.sum(tile, axis=0, keepdims=True), axis=1, keepdims=True)
            packed = jnp.where(jnp.logical_and(row == n % 8, lane == n // 8), value, packed)
        for k in range(copies):
            out[k] = packed

    return on_core(body, [(copies, 8, width)], *basis)[0]


def add(a, b):
    return b if a is None else a if b is None else a + b


def times(s, vec):
    return {i: s * v for i, v in vec.items()}


def plus(u, v):
    return {i: add(u.get(i), v.get(i)) for i in sorted(set(u) | set(v))}


def iterations(count, gram, applied, residual, direction, norm, gain):
    def dot(u, v):
        out = None
        for i, a in u.items():
            part = None
            for j, b in v.items():
                part = add(part, gram[i, j] * b)
            out = add(out, a * part)
        return out

    log = []
    for step in range(count):
        image = applied(direction)
        alpha = norm / dot(direction, image)
        gain = plus(gain, times(alpha, direction))
        residual = plus(residual, times(-alpha, image))
        last = direction
        if step + 1 < count:
            norm_next = dot(residual, residual)
            log.append((alpha, norm_next / norm, norm))
            direction = plus(residual, times(norm_next / norm, direction))
            norm = norm_next
        else:
            log.append((alpha, None, norm))
    return gain, residual, last, log


def gram_of(sums_ref, count, tile):
    total = sums_ref[0]
    for k in range(1, sums_ref.shape[0]):
        total = total + sums_ref[k]
    gram = {}
    for n, (i, j) in enumerate(pairs_of(count)):
        value = jnp.broadcast_to(total[n % 8 : n % 8 + 1, n // 8 : n // 8 + 1], tile)
        gram[i, j] = gram[j, i] = value
    return gram


def first_update(sums, basis):
    shape = basis[0].shape
    tile = shape[1:]

    def body(sums_ref, v0, v1, v2, state_out, r_out):
        gram = gram_of(sums_ref, 3, tile)

        def applied(u):
            return {i + 1: a * (1.0 / SCALE) for i, a in u.items()}

        start = {0: jnp.ones(tile, jnp.float32)}
        gain, residual, direction, log = iterations(
            FIRST, gram, applied, start, start, gram[0, 0], {}
        )
        (alpha0, beta0, _), (alpha1, _, norm) = log
        centre = 1.0 / alpha1 + beta0 / alpha0
        spread_ = jnp.maximum(jnp.sqrt(jnp.maximum(beta0, 0.0)) / alpha0, 1e-3 * centre)
        kept = (
            norm, direction[0], direction[1], gain[0], gain[1],
            residual[0], residual[1], residual[2], centre, spread_, 1.0 / spread_,
        )
        for n, value in enumerate(kept):
            state_out[n] = value
        for c in range(shape[0]):
            r_out[c] = residual[0] * v0[c] + residual[1] * v1[c] + residual[2] * v2[c]

    return on_core(body, [(STATE,) + tile, shape], sums, *basis)


STATE = 11
CENTRE, WIDTH, INVERSE = (8, 9, 10)


def last_update(sums, state, basis):
    shape = basis[0].shape
    tile = shape[1:]
    count = len(basis)

    def body(sums_ref, state_ref, *refs):
        vectors, x_out = (refs[:-1], refs[-1])
        gram = gram_of(sums_ref, count, tile)
        kept = [state_ref[n] for n in range(STATE)]
        norm_before, p0, p1, g0, g1, c0, c1, c2, centre, width, _ = kept
        share = (1.0 / SCALE) / c2
        second = {0: -share * c0, 1: -share * c1, 2: share}

        def applied(u):
            out = {}
            for i, a in u.items():
                if i == 0:
                    out = plus(out, {1: a * (1.0 / SCALE)})
                elif i == 1:
                    out = plus(out, times(a, second))
                else:
                    wide = a * width
                    out = plus(out, {i: a * centre, i + 1: wide})
                    if i > 2:
                        out = plus(out, {i - 1: wide})
            return out

        one = jnp.ones(tile, jnp.float32)
        norm = gram[2, 2]
        ratio = norm / norm_before
        direction = {0: ratio * p0, 1: ratio * p1, 2: one}
        gain, _, _, _ = iterations(
            ITERS - FIRST, gram, applied, {2: one}, direction, norm, {0: g0, 1: g1}
        )
        for c in range(shape[0]):
            x_out[c] = sum(s * vectors[i][c] for i, s in gain.items())

    return on_core(body, [shape], sums, state, *basis)[0]


def per_device(source, fat_links, long_links):
    rows, depth, width = source.shape[2:]
    dims = (rows, depth, width)
    tile = (rows * depth, width)
    field = source.reshape((6,) + tile)
    fat = fat_links.reshape((2, 4, 18) + tile)
    long = long_links.reshape((2, 4, 18) + tile)
    near = [
        passed_along(jnp.stack([fat[:, mu], long[:, mu]]), axis, 1)
        for mu, axis in enumerate(AXES)
    ]
    odd_table = link_table(fat, long, near, dims, 1)
    even_table = link_table(fat, long, near, dims, 0)
    even = jnp.stack([lax.axis_index(axis) % 2 == 0 for axis in AXES])
    flags = jnp.broadcast_to(even.astype(jnp.float32)[:, None, None], (len(AXES),) + tile)

    devices = 1
    for size in axis_sizes():
        devices *= size

    def image(vector, finish, *extra):
        odd = odd_from_even(vector, odd_table, flags, dims)
        return even_from_odd(odd, vector, even_table, flags, dims, finish, *extra)

    def summed(basis):
        return lax.all_to_all(gram_parts(basis, devices), AXES, 0, 0, tiled=True)

    def scaled(c, value, vector, more):
        return SCALE * value

    def shifted(c, value, vector, more):
        state = more[0]
        value = (value - state[CENTRE] * vector[c]) * state[INVERSE]
        return value - more[1][c] if len(more) > 1 else value

    def remaining(c, value, vector, more):
        return more[0][c] - value

    basis = [field]
    for _ in range(FIRST):
        basis.append(image(basis[-1], scaled))
    state, residual = first_update(summed(basis), basis)
    basis = basis[:FIRST] + [residual]
    for step in range(ITERS - FIRST):
        basis.append(image(basis[-1], shifted, state, *([basis[-2]] if step else [])))
    solution = last_update(summed(basis), state, basis)
    true = image(solution, remaining, field)
    return (solution.reshape(source.shape), true.reshape(source.shape))


def solution(mesh):
    in_specs = (
        P(None, None, "ta", "gz", "gy"),
        P(None, None, None, None, None, "ta", "gz", "gy"),
        P(None, None, None, None, None, "ta", "gz", "gy"),
    )
    out_specs = (P(None, None, "ta", "gz", "gy"), P(None, None, "ta", "gz", "gy"))
    return jax.shard_map(
        per_device, mesh=mesh, in_specs=in_specs, out_specs=out_specs, check_vma=False
    )
```

```python
import jax
import jax.numpy as jnp
from jax import lax
from jax.experimental import pallas as pl
from jax.experimental.pallas import tpu as pltpu
from jax.sharding import PartitionSpec as P

NX = 32
ITERS = 8
FIRST = 2


mass_squared = 0.1
SCALE = 1.0 / 16.0

VMEM = pl.BlockSpec(memory_space=pltpu.VMEM)
PARAMS = pltpu.CompilerParams(vmem_limit_bytes=4 * 2**20)
AXES = ("ta", "gz", "gy")


def on_core(body, outs, *args):
    return pl.pallas_call(
        body,
        out_shape=tuple(jax.ShapeDtypeStruct(shape, jnp.float32) for shape in outs),
        in_specs=[VMEM] * len(args),
        out_specs=tuple(VMEM for _ in outs),
        compiler_params=PARAMS,
    )(*args)


def passed_along(shard, axis, by):
    size = lax.axis_size(axis)
    return lax.ppermute(shard, axis, [(i, (i + by) % size) for i in range(size)])


def swapped(shard, axis, odd):
    size = lax.axis_size(axis)
    assert size % 2 == 0
    ahead = [(i, (i + 1) % size) for i in range(odd, size, 2)]
    return lax.ppermute(shard, axis, ahead + [(j, i) for i, j in ahead])


def rolled(tile, shift, axis):
    shift = shift % tile.shape[axis]
    return pltpu.roll(tile, shift, axis) if shift else tile


class Shifts:
    def __init__(self, rows, depth, width):
        self.rows, self.depth, self.width = (rows, depth, width)
        self.shape = (rows * depth, width)
        sub = lax.broadcasted_iota(jnp.int32, self.shape, 0)
        self.lane = lax.broadcasted_iota(jnp.int32, self.shape, 1)
        self.row = sub // depth
        self.plane = sub % depth
        self.x = self.lane % NX
        self.odd = (self.plane + self.lane // NX + self.x) % 2 == 1

    def select(self, dst):
        return self.odd if dst == 0 else jnp.logical_not(self.odd)

    def t_rows(self, own, other, by):
        if by == 0:
            return own
        near = self.row >= by if by > 0 else self.row < self.rows + by
        return rolled(jnp.where(near, own, other), -by * self.depth, 0)

    def t(self, own, other, by, dst):
        sel = self.select(dst)
        half = {1: (1, 0), 3: (2, 1), -1: (0, -1), -3: (-1, -2)}[by]
        return jnp.where(sel, self.t_rows(own, other, half[0]), self.t_rows(own, other, half[1]))

    def z(self, own, other, by):
        near = self.plane < self.depth - by if by > 0 else self.plane >= -by
        wrap = self.depth - by if by > 0 else -self.depth - by
        return jnp.where(near, rolled(own, -by, 0), rolled(other, wrap, 0))

    def y(self, own, other, by):
        lanes = by * NX
        near = self.lane >= lanes if by > 0 else self.lane < self.width + lanes
        return rolled(jnp.where(near, own, other), -lanes, 1)

    def x_(self, own, by):
        near = self.x < NX - by if by > 0 else self.x >= -by
        wrap = NX - by if by > 0 else -NX - by
        return jnp.where(near, rolled(own, -by, 1), rolled(own, wrap, 1))

    def hop(self, own, other, mu, by, dst):
        if mu == 0:
            return self.t(own, other, by, dst)
        if mu == 1:
            return self.z(own, other, by)
        if mu == 2:
            return self.y(own, other, by)
        return self.x_(own, by)


HOPS = tuple((mu, by) for mu in range(4) for by in (1, 3, -1, -3))


def link_table(fat, long, near, dims, dst):
    rows, depth, width = dims
    tile = (rows * depth, width)

    def body(fat_ref, long_ref, t_ref, z_ref, y_ref, out):
        shifts = Shifts(rows, depth, width)
        lows = (t_ref, z_ref, y_ref)

        def entry(i, carry):
            flip = 3 * (i % 3) + i // 3
            for k, (mu, by) in enumerate(HOPS):
                kind = 0 if abs(by) == 1 else 1
                ref = (fat_ref, long_ref)[kind]
                for part in range(2):
                    if by > 0:
                        value = ref[dst, mu, 9 * part + i].astype(jnp.float32)
                        out[18 * k + 9 * part + i] = value
                    else:
                        own = ref[1 - dst, mu, 9 * part + i].astype(jnp.float32)
                        other = own
                        if mu < 3:
                            other = lows[mu][kind, 1 - dst, 9 * part + i].astype(jnp.float32)
                        value = shifts.hop(own, other, mu, by, dst)
                        out[18 * k + 9 * part + flip] = value if part else -value
            return carry

        lax.fori_loop(0, 9, entry, 0)

    return on_core(body, [(18 * len(HOPS),) + tile], fat, long, *near)[0]


def hopping_sum(shifts, field, near, table, dst):
    flags = near[-1]
    total = [None] * 6
    for mu in range(4):
        ahead = behind = [None] * 6
        if mu < 3:
            one, two = (near[2 * mu], near[2 * mu + 1])
            if one is two:
                ahead = behind = [one[c] for c in range(6)]
            else:
                even = flags[mu] > 0.5
                pairs = [(one[c], two[c]) for c in range(6)]
                ahead = [jnp.where(even, u, v) for u, v in pairs]
                behind = [jnp.where(even, v, u) for u, v in pairs]
        for k, (axis, by) in enumerate(HOPS):
            if axis != mu:
                continue
            other = ahead if by > 0 else behind
            hopped = [shifts.hop(field[c], other[c], mu, by, dst) for c in range(6)]
            for a in range(3):
                re = im = None
                for b in range(3):
                    lre = table[18 * k + 3 * a + b]
                    lim = table[18 * k + 9 + 3 * a + b]
                    vre, vim = (hopped[b], hopped[3 + b])
                    x, y = (lre * vre - lim * vim, lre * vim + lim * vre)
                    re = x if re is None else re + x
                    im = y if im is None else im + y
                total[a] = re if total[a] is None else total[a] + re
                total[3 + a] = im if total[3 + a] is None else total[3 + a] + im
    return total


def axis_sizes():
    return tuple(lax.axis_size(axis) for axis in AXES)


def swaps_of(sizes):
    return tuple(
        (mu, odd) for odd in (1, 0) for mu in (2, 0, 1) if odd == 0 or sizes[mu] > 2
    )


def neighbours(field):
    return tuple(swapped(field, AXES[mu], odd) for mu, odd in swaps_of(axis_sizes()))


def spread(refs, sizes):
    keys = swaps_of(sizes)
    got = dict(zip(keys, refs))
    near = [got.get((mu, odd), got[mu, 0]) for mu in range(3) for odd in (0, 1)]
    return near, list(refs[len(keys) :])


def odd_from_even(field, near, table, flags, dims):
    sizes = axis_sizes()

    def body(field_ref, table_ref, flags_ref, *refs):
        others, (out,) = spread(refs, sizes)
        shifts = Shifts(*dims)
        terms = hopping_sum(shifts, field_ref, others + [flags_ref], table_ref, 1)
        for c, value in enumerate(terms):
            out[c] = value

    return on_core(body, [field.shape], field, table, flags, *near)[0]


def even_from_odd(field, near, start, table, flags, dims, finish, *extra):
    sizes = axis_sizes()

    def body(field_ref, start_ref, table_ref, flags_ref, *refs):
        others, rest = spread(refs, sizes)
        more, out = (rest[:-1], rest[-1])
        shifts = Shifts(*dims)
        terms = hopping_sum(shifts, field_ref, others + [flags_ref], table_ref, 0)
        for c, value in enumerate(terms):
            out[c] = finish(c, mass_squared * start_ref[c] - value, start_ref, more)

    return on_core(body, [field.shape], field, start, table, flags, *near, *extra)[0]


def pairs_of(count):
    return tuple((i, j) for i in range(count) for j in range(i, count)) + ((count, count),)


def gram_parts(basis, odd, copies):
    fields = tuple(basis) + (odd,)
    parts, width = odd.shape[0], 128

    def body(*refs):
        out = refs[-1]
        lane = lax.broadcasted_iota(jnp.int32, (1, width), 1)
        packed = jnp.zeros((1, width), jnp.float32)
        for n, (i, j) in enumerate(pairs_of(len(basis))):
            tile = refs[i][0] * refs[j][0]
            for c in range(1, parts):
                tile = tile + refs[i][c] * refs[j][c]
            value = jnp.sum(jnp.sum(tile, axis=0, keepdims=True), axis=1, keepdims=True)
            packed = jnp.where(lane == n, value, packed)
        for k in range(copies):
            out[k] = packed

    return on_core(body, [(copies, 1, width)], *fields)[0]


def add(a, b):
    return b if a is None else a if b is None else a + b


def times(s, vec):
    return {i: s * v for i, v in vec.items()}


def plus(u, v):
    return {i: add(u.get(i), v.get(i)) for i in sorted(set(u) | set(v))}


def iterations(count, gram, applied, residual, direction, norm, gain):
    def dot(u, v):
        out = None
        for i, a in u.items():
            part = None
            for j, b in v.items():
                part = add(part, gram[i, j] * b)
            out = add(out, a * part)
        return out

    log = []
    for step in range(count):
        image = applied(direction)
        alpha = norm / dot(direction, image)
        gain = plus(gain, times(alpha, direction))
        residual = plus(residual, times(-alpha, image))
        last = direction
        if step + 1 < count:
            norm_next = dot(residual, residual)
            log.append((alpha, norm_next / norm, norm))
            direction = plus(residual, times(norm_next / norm, direction))
            norm = norm_next
        else:
            log.append((alpha, None, norm))
    return gain, residual, last, log


def gram_of(sums_ref, count, tile, applied):
    total = sums_ref[0]
    for k in range(1, sums_ref.shape[0]):
        total = total + sums_ref[k]
    gram = {}
    for n, (i, j) in enumerate(pairs_of(count)):
        value = jnp.broadcast_to(total[:, n : n + 1], tile)
        gram[i, j] = gram[j, i] = value
    last = count - 1
    square = gram.pop((count, count))
    one = jnp.ones(tile, jnp.float32)
    image = applied({last: one})
    top = image.pop(count)
    for i in range(count):
        if i < last:
            product = sum(b * gram[k, last] for k, b in applied({i: one}).items())
        else:
            product = mass_squared * gram[last, last] + square
        for k, b in image.items():
            product = product - b * gram[i, k]
        gram[i, count] = gram[count, i] = product / top
    return gram


def first_update(sums, basis):
    shape = basis[0].shape
    tile = shape[1:]

    def body(sums_ref, v0, v1, v2, state_out, r_out):
        def applied(u):
            return {i + 1: a * (1.0 / SCALE) for i, a in u.items()}

        gram = gram_of(sums_ref, FIRST, tile, applied)
        start = {0: jnp.ones(tile, jnp.float32)}
        gain, residual, direction, log = iterations(
            FIRST, gram, applied, start, start, gram[0, 0], {}
        )
        (alpha0, beta0, _), (alpha1, _, norm) = log
        centre = 1.0 / alpha1 + beta0 / alpha0
        width = jnp.maximum(jnp.sqrt(jnp.maximum(beta0, 0.0)) / alpha0, 1e-3 * centre)
        kept = (
            norm, direction[0], direction[1], gain[0], gain[1],
            residual[0], residual[1], residual[2], centre, width, 1.0 / width,
        )
        for n, value in enumerate(kept):
            state_out[n] = value
        for c in range(shape[0]):
            r_out[c] = residual[0] * v0[c] + residual[1] * v1[c] + residual[2] * v2[c]

    return on_core(body, [(STATE,) + tile, shape], sums, *basis)


STATE = 11
CENTRE, INVERSE = (8, 10)


def last_update(sums, state, basis):
    shape = basis[0].shape
    tile = shape[1:]
    count = len(basis)

    def body(sums_ref, state_ref, *refs):
        vectors, x_out = (refs[:-1], refs[-1])
        kept = [state_ref[n] for n in range(STATE)]
        norm_before, p0, p1, g0, g1, c0, c1, c2, centre, width, _ = kept
        share = (1.0 / SCALE) / c2
        second = {0: -share * c0, 1: -share * c1, 2: share}

        def applied(u):
            out = {}
            for i, a in u.items():
                if i == 0:
                    out = plus(out, {1: a * (1.0 / SCALE)})
                elif i == 1:
                    out = plus(out, times(a, second))
                else:
                    wide = a * width
                    out = plus(out, {i: a * centre, i + 1: wide})
                    if i > 2:
                        out = plus(out, {i - 1: wide})
            return out

        gram = gram_of(sums_ref, count, tile, applied)
        one = jnp.ones(tile, jnp.float32)
        norm = gram[2, 2]
        ratio = norm / norm_before
        direction = {0: ratio * p0, 1: ratio * p1, 2: one}
        gain, _, _, _ = iterations(
            ITERS - FIRST, gram, applied, {2: one}, direction, norm, {0: g0, 1: g1}
        )
        for c in range(shape[0]):
            x_out[c] = sum(s * vectors[i][c] for i, s in gain.items())

    return on_core(body, [shape], sums, state, *basis)[0]


def per_device(source, fat_links, long_links):
    rows, depth, width = source.shape[2:]
    dims = (rows, depth, width)
    tile = (rows * depth, width)
    field = source.reshape((6,) + tile)
    fat = fat_links.reshape((2, 4, 18) + tile)
    long = long_links.reshape((2, 4, 18) + tile)
    near = {
        mu: passed_along(jnp.stack([fat[:, mu], long[:, mu]]), AXES[mu], 1) for mu in (2, 0, 1)
    }
    near = [near[mu] for mu in range(3)]
    odd_table = link_table(fat, long, near, dims, 1)
    even_table = link_table(fat, long, near, dims, 0)
    even = jnp.stack([lax.axis_index(axis) % 2 == 0 for axis in AXES])
    flags = jnp.broadcast_to(even.astype(jnp.float32)[:, None, None], (len(AXES),) + tile)

    devices = 1
    for size in axis_sizes():
        devices *= size

    def half(vector):
        return odd_from_even(vector, neighbours(vector), odd_table, flags, dims)

    def image(vector, odd, near, finish, *extra):
        return even_from_odd(odd, near, vector, even_table, flags, dims, finish, *extra)

    def summed(basis, odd):
        return lax.all_to_all(gram_parts(basis, odd, devices), AXES, 0, 0, tiled=True)

    def scaled(c, value, vector, more):
        return SCALE * value

    def shifted(c, value, vector, more):
        state = more[0]
        value = (value - state[CENTRE] * vector[c]) * state[INVERSE]
        return value - more[1][c] if len(more) > 1 else value

    def remaining(c, value, vector, more):
        return more[0][c] - value

    basis = [field]
    odd = half(field)
    for _ in range(FIRST - 1):
        basis.append(image(basis[-1], odd, neighbours(odd), scaled))
        odd = half(basis[-1])
    near = neighbours(odd)
    sums = summed(basis, odd)
    basis.append(image(basis[-1], odd, near, scaled))
    state, residual = first_update(sums, basis)
    basis = basis[:FIRST] + [residual]
    odd = half(residual)
    for step in range(ITERS - FIRST - 1):
        before = [basis[-2]] if step else []
        basis.append(image(basis[-1], odd, neighbours(odd), shifted, state, *before))
        odd = half(basis[-1])
    solution = last_update(summed(basis, odd), state, basis)
    final = half(solution)
    true = image(solution, final, neighbours(final), remaining, field)
    return (solution.reshape(source.shape), true.reshape(source.shape))


def solution(mesh):
    in_specs = (
        P(None, None, "ta", "gz", "gy"),
        P(None, None, None, None, None, "ta", "gz", "gy"),
        P(None, None, None, None, None, "ta", "gz", "gy"),
    )
    out_specs = (P(None, None, "ta", "gz", "gy"), P(None, None, "ta", "gz", "gy"))
    return jax.shard_map(
        per_device, mesh=mesh, in_specs=in_specs, out_specs=out_specs, check_vma=False
    )
```

```python
import jax
import jax.numpy as jnp
from jax import lax
from jax.experimental import pallas as pl
from jax.experimental.pallas import tpu as pltpu
from jax.sharding import PartitionSpec as P

NX = 32
ITERS = 8
FIRST = 2


mass_squared = 0.1
SCALE = 1.0 / 16.0

VMEM = pl.BlockSpec(memory_space=pltpu.VMEM)
PARAMS = pltpu.CompilerParams(vmem_limit_bytes=4 * 2**20)
AXES = ("ta", "gz", "gy")


def on_core(body, outs, *args):
    return pl.pallas_call(
        body,
        out_shape=tuple(jax.ShapeDtypeStruct(shape, jnp.float32) for shape in outs),
        in_specs=[VMEM] * len(args),
        out_specs=tuple(VMEM for _ in outs),
        compiler_params=PARAMS,
    )(*args)


def passed_along(shard, axis, by):
    size = lax.axis_size(axis)
    return lax.ppermute(shard, axis, [(i, (i + by) % size) for i in range(size)])


def swapped(shard, axis, odd):
    size = lax.axis_size(axis)
    assert size % 2 == 0
    ahead = [(i, (i + 1) % size) for i in range(odd, size, 2)]
    return lax.ppermute(shard, axis, ahead + [(j, i) for i, j in ahead])


def rolled(tile, shift, axis):
    shift = shift % tile.shape[axis]
    return pltpu.roll(tile, shift, axis) if shift else tile


class Shifts:
    def __init__(self, rows, depth, width):
        self.rows, self.depth, self.width = (rows, depth, width)
        self.shape = (rows * depth, width)
        sub = lax.broadcasted_iota(jnp.int32, self.shape, 0)
        self.lane = lax.broadcasted_iota(jnp.int32, self.shape, 1)
        self.row = sub // depth
        self.plane = sub % depth
        self.x = self.lane % NX
        self.odd = (self.plane + self.lane // NX + self.x) % 2 == 1

    def select(self, dst):
        return self.odd if dst == 0 else jnp.logical_not(self.odd)

    def t_rows(self, own, other, by):
        if by == 0:
            return own
        near = self.row >= by if by > 0 else self.row < self.rows + by
        return rolled(jnp.where(near, own, other), -by * self.depth, 0)

    def t(self, own, other, by, dst):
        sel = self.select(dst)
        half = {1: (1, 0), 3: (2, 1), -1: (0, -1), -3: (-1, -2)}[by]
        return jnp.where(sel, self.t_rows(own, other, half[0]), self.t_rows(own, other, half[1]))

    def z(self, own, other, by):
        near = self.plane < self.depth - by if by > 0 else self.plane >= -by
        wrap = self.depth - by if by > 0 else -self.depth - by
        return jnp.where(near, rolled(own, -by, 0), rolled(other, wrap, 0))

    def y(self, own, other, by):
        lanes = by * NX
        near = self.lane >= lanes if by > 0 else self.lane < self.width + lanes
        return rolled(jnp.where(near, own, other), -lanes, 1)

    def x_(self, own, by):
        near = self.x < NX - by if by > 0 else self.x >= -by
        wrap = NX - by if by > 0 else -NX - by
        return jnp.where(near, rolled(own, -by, 1), rolled(own, wrap, 1))

    def hop(self, own, other, mu, by, dst):
        if mu == 0:
            return self.t(own, other, by, dst)
        if mu == 1:
            return self.z(own, other, by)
        if mu == 2:
            return self.y(own, other, by)
        return self.x_(own, by)


HOPS = tuple((mu, by) for mu in range(4) for by in (1, 3, -1, -3))


def link_table(fat, long, near, dims, dst):
    rows, depth, width = dims
    tile = (rows * depth, width)

    def body(fat_ref, long_ref, t_ref, z_ref, y_ref, out):
        shifts = Shifts(rows, depth, width)
        lows = (t_ref, z_ref, y_ref)

        def flat(block):
            return block.astype(jnp.float32).reshape(tile)

        def entry(i, carry):
            flip = 3 * (i % 3) + i // 3
            for k, (mu, by) in enumerate(HOPS):
                kind = 0 if abs(by) == 1 else 1
                ref = (fat_ref, long_ref)[kind]
                for part in range(2):
                    if by > 0:
                        value = flat(ref[dst, mu, part, i // 3, i % 3])
                        out[18 * k + 9 * part + i] = value
                    else:
                        own = flat(ref[1 - dst, mu, part, i // 3, i % 3])
                        other = own
                        if mu < 3:
                            other = flat(lows[mu][kind, 1 - dst, part, i // 3, i % 3])
                        value = shifts.hop(own, other, mu, by, dst)
                        out[18 * k + 9 * part + flip] = value if part else -value
            return carry

        lax.fori_loop(0, 9, entry, 0)

    return on_core(body, [(18 * len(HOPS),) + tile], fat, long, *near)[0]


def hopping_sum(shifts, field, near, table, dst):
    flags = near[-1]
    total = [None] * 6
    for mu in range(4):
        ahead = behind = [None] * 6
        if mu < 3:
            one, two = (near[2 * mu], near[2 * mu + 1])
            if one is two:
                ahead = behind = [one[c] for c in range(6)]
            else:
                even = flags[mu] > 0.5
                pairs = [(one[c], two[c]) for c in range(6)]
                ahead = [jnp.where(even, u, v) for u, v in pairs]
                behind = [jnp.where(even, v, u) for u, v in pairs]
        for k, (axis, by) in enumerate(HOPS):
            if axis != mu:
                continue
            other = ahead if by > 0 else behind
            hopped = [shifts.hop(field[c], other[c], mu, by, dst) for c in range(6)]
            for a in range(3):
                re = im = None
                for b in range(3):
                    lre = table[18 * k + 3 * a + b]
                    lim = table[18 * k + 9 + 3 * a + b]
                    vre, vim = (hopped[b], hopped[3 + b])
                    x, y = (lre * vre - lim * vim, lre * vim + lim * vre)
                    re = x if re is None else re + x
                    im = y if im is None else im + y
                total[a] = re if total[a] is None else total[a] + re
                total[3 + a] = im if total[3 + a] is None else total[3 + a] + im
    return total


def axis_sizes():
    return tuple(lax.axis_size(axis) for axis in AXES)


def swaps_of(sizes):
    return tuple(
        (mu, odd) for odd in (1, 0) for mu in (2, 0, 1) if odd == 0 or sizes[mu] > 2
    )


def neighbours(field):
    return tuple(swapped(field, AXES[mu], odd) for mu, odd in swaps_of(axis_sizes()))


def spread(refs, sizes):
    keys = swaps_of(sizes)
    got = dict(zip(keys, refs))
    near = [got.get((mu, odd), got[mu, 0]) for mu in range(3) for odd in (0, 1)]
    return near, list(refs[len(keys) :])


def odd_from_even(field, near, table, flags, dims):
    sizes = axis_sizes()

    def body(field_ref, table_ref, flags_ref, *refs):
        others, (out,) = spread(refs, sizes)
        shifts = Shifts(*dims)
        terms = hopping_sum(shifts, field_ref, others + [flags_ref], table_ref, 1)
        for c, value in enumerate(terms):
            out[c] = value

    return on_core(body, [field.shape], field, table, flags, *near)[0]


def even_from_odd(field, near, start, table, flags, dims, finish, *extra):
    sizes = axis_sizes()

    def body(field_ref, start_ref, table_ref, flags_ref, *refs):
        others, rest = spread(refs, sizes)
        more, out = (rest[:-1], rest[-1])
        shifts = Shifts(*dims)
        terms = hopping_sum(shifts, field_ref, others + [flags_ref], table_ref, 0)
        for c, value in enumerate(terms):
            out[c] = finish(value, start_ref[c], c, more)

    return on_core(body, [field.shape], field, start, table, flags, *near, *extra)[0]


def pairs_of(count):
    return tuple((i, j) for i in range(count) for j in range(i, count)) + ((count, count),)


def gram_parts(basis, odd, copies):
    fields = tuple(basis) + (odd,)
    parts, width = odd.shape[0], 128

    def body(*refs):
        out = refs[-1]
        lane = lax.broadcasted_iota(jnp.int32, (1, width), 1)
        packed = jnp.zeros((1, width), jnp.float32)
        for n, (i, j) in enumerate(pairs_of(len(basis))):
            tile = refs[i][0] * refs[j][0]
            for c in range(1, parts):
                tile = tile + refs[i][c] * refs[j][c]
            value = jnp.sum(jnp.sum(tile, axis=0, keepdims=True), axis=1, keepdims=True)
            packed = jnp.where(lane == n, value, packed)
        for k in range(copies):
            out[k] = packed

    return on_core(body, [(copies, 1, width)], *fields)[0]


def add(a, b):
    return b if a is None else a if b is None else a + b


def times(s, vec):
    return {i: s * v for i, v in vec.items()}


def plus(u, v):
    return {i: add(u.get(i), v.get(i)) for i in sorted(set(u) | set(v))}


def iterations(count, gram, applied, residual, direction, norm, gain):
    def dot(u, v):
        out = None
        for i, a in u.items():
            part = None
            for j, b in v.items():
                part = add(part, gram[i, j] * b)
            out = add(out, a * part)
        return out

    log = []
    for step in range(count):
        image = applied(direction)
        alpha = norm / dot(direction, image)
        gain = plus(gain, times(alpha, direction))
        residual = plus(residual, times(-alpha, image))
        last = direction
        if step + 1 < count:
            norm_next = dot(residual, residual)
            log.append((alpha, norm_next / norm, norm))
            direction = plus(residual, times(norm_next / norm, direction))
            norm = norm_next
        else:
            log.append((alpha, None, norm))
    return gain, residual, last, log


def gram_of(sums_ref, count, tile, applied):
    total = sums_ref[0]
    for k in range(1, sums_ref.shape[0]):
        total = total + sums_ref[k]
    gram = {}
    for n, (i, j) in enumerate(pairs_of(count)):
        value = jnp.broadcast_to(total[:, n : n + 1], tile)
        gram[i, j] = gram[j, i] = value
    last = count - 1
    square = gram.pop((count, count))
    one = jnp.ones(tile, jnp.float32)
    image = applied({last: one})
    top = image.pop(count)
    for i in range(count):
        if i < last:
            product = sum(b * gram[k, last] for k, b in applied({i: one}).items())
        else:
            product = mass_squared * gram[last, last] + square
        for k, b in image.items():
            product = product - b * gram[i, k]
        gram[i, count] = gram[count, i] = product / top
    return gram


def first_update(sums, basis):
    shape = basis[0].shape
    tile = shape[1:]

    def body(sums_ref, v0, v1, v2, state_out, r_out):
        def applied(u):
            return {i + 1: a * (1.0 / SCALE) for i, a in u.items()}

        gram = gram_of(sums_ref, FIRST, tile, applied)
        start = {0: jnp.ones(tile, jnp.float32)}
        gain, residual, direction, log = iterations(
            FIRST, gram, applied, start, start, gram[0, 0], {}
        )
        (alpha0, beta0, _), (alpha1, _, norm) = log
        centre = 1.0 / alpha1 + beta0 / alpha0
        width = jnp.maximum(jnp.sqrt(jnp.maximum(beta0, 0.0)) / alpha0, 1e-3 * centre)
        kept = (
            norm, direction[0], direction[1], gain[0], gain[1],
            residual[0], residual[1], residual[2], centre, width, 1.0 / width,
        )
        for n, value in enumerate(kept):
            state_out[n] = value
        for c in range(shape[0]):
            r_out[c] = residual[0] * v0[c] + residual[1] * v1[c] + residual[2] * v2[c]

    return on_core(body, [(STATE,) + tile, shape], sums, *basis)


STATE = 11
CENTRE, INVERSE = (8, 10)


def last_update(sums, state, basis, odds):
    shape = basis[0].shape
    tile = shape[1:]
    count = len(basis)

    def body(sums_ref, state_ref, *refs):
        vectors, images = (refs[:count], refs[count : 2 * count])
        x_out, odd_out, rest_out = refs[2 * count :]
        kept = [state_ref[n] for n in range(STATE)]
        norm_before, p0, p1, g0, g1, c0, c1, c2, centre, width, _ = kept
        share = (1.0 / SCALE) / c2
        second = {0: -share * c0, 1: -share * c1, 2: share}

        def applied(u):
            out = {}
            for i, a in u.items():
                if i == 0:
                    out = plus(out, {1: a * (1.0 / SCALE)})
                elif i == 1:
                    out = plus(out, times(a, second))
                else:
                    wide = a * width
                    out = plus(out, {i: a * centre, i + 1: wide})
                    if i > 2:
                        out = plus(out, {i - 1: wide})
            return out

        gram = gram_of(sums_ref, count, tile, applied)
        one = jnp.ones(tile, jnp.float32)
        norm = gram[2, 2]
        ratio = norm / norm_before
        direction = {0: ratio * p0, 1: ratio * p1, 2: one}
        gain, _, _, _ = iterations(
            ITERS - FIRST, gram, applied, {2: one}, direction, norm, {0: g0, 1: g1}
        )
        for c in range(shape[0]):
            total = sum(s * vectors[i][c] for i, s in gain.items())
            x_out[c] = total
            rest_out[c] = vectors[0][c] - mass_squared * total
            odd_out[c] = sum(s * images[i][c] for i, s in gain.items())

    return on_core(body, [shape] * 3, sums, state, *basis, *odds)


def per_device(source, fat_links, long_links):
    rows, depth, width = source.shape[2:]
    dims = (rows, depth, width)
    tile = (rows * depth, width)
    field = source.reshape((6,) + tile)
    fat, long = (fat_links, long_links)
    near = {
        mu: passed_along(jnp.stack([fat[:, mu], long[:, mu]]), AXES[mu], 1) for mu in (2, 0, 1)
    }
    near = [near[mu] for mu in range(3)]
    odd_table = link_table(fat, long, near, dims, 1)
    even_table = link_table(fat, long, near, dims, 0)
    even = jnp.stack([lax.axis_index(axis) % 2 == 0 for axis in AXES])
    flags = jnp.broadcast_to(even.astype(jnp.float32)[:, None, None], (len(AXES),) + tile)

    devices = 1
    for size in axis_sizes():
        devices *= size

    def half(vector):
        return odd_from_even(vector, neighbours(vector), odd_table, flags, dims)

    def image(vector, odd, near, finish, *extra):
        return even_from_odd(odd, near, vector, even_table, flags, dims, finish, *extra)

    def summed(basis, odd):
        return lax.all_to_all(gram_parts(basis, odd, devices), AXES, 0, 0, tiled=True)

    def scaled(value, vector, c, more):
        return SCALE * (mass_squared * vector - value)

    def shifted(value, vector, c, more):
        state = more[0]
        value = ((mass_squared - state[CENTRE]) * vector - value) * state[INVERSE]
        return value - more[1][c] if len(more) > 1 else value

    def remaining(value, rest, c, more):
        return rest + value

    basis, odds = ([field], [half(field)])
    for _ in range(FIRST - 1):
        basis.append(image(basis[-1], odds[-1], neighbours(odds[-1]), scaled))
        odds.append(half(basis[-1]))
    near = neighbours(odds[-1])
    sums = summed(basis, odds[-1])
    last = image(basis[-1], odds[-1], near, scaled)
    state, residual = first_update(sums, basis + [last])
    basis.append(residual)
    odds.append(half(residual))
    for step in range(ITERS - FIRST - 1):
        before = [basis[-2]] if step else []
        near = neighbours(odds[-1])
        basis.append(image(basis[-1], odds[-1], near, shifted, state, *before))
        odds.append(half(basis[-1]))
    solution, odd, rest = last_update(summed(basis, odds[-1]), state, basis, odds)
    true = image(rest, odd, neighbours(odd), remaining)
    return (solution.reshape(source.shape), true.reshape(source.shape))


def solution(mesh):
    in_specs = (
        P(None, None, "ta", "gz", "gy"),
        P(None, None, None, None, None, "ta", "gz", "gy"),
        P(None, None, None, None, None, "ta", "gz", "gy"),
    )
    out_specs = (P(None, None, "ta", "gz", "gy"), P(None, None, "ta", "gz", "gy"))
    return jax.shard_map(
        per_device, mesh=mesh, in_specs=in_specs, out_specs=out_specs, check_vma=False
    )
```

```python
import jax
import jax.numpy as jnp
from jax import lax
from jax.experimental import pallas as pl
from jax.experimental.pallas import tpu as pltpu
from jax.sharding import PartitionSpec as P

NX = 32
ITERS = 8
FIRST = 2


mass_squared = 0.1
SCALE = 1.0 / 16.0

VMEM = pl.BlockSpec(memory_space=pltpu.VMEM)
PARAMS = pltpu.CompilerParams(vmem_limit_bytes=4 * 2**20)
AXES = ("ta", "gz", "gy")


def on_core(body, outs, *args):
    return pl.pallas_call(
        body,
        out_shape=tuple(jax.ShapeDtypeStruct(shape, jnp.float32) for shape in outs),
        in_specs=[VMEM] * len(args),
        out_specs=tuple(VMEM for _ in outs),
        compiler_params=PARAMS,
    )(*args)


def passed_along(shard, axis, by):
    size = lax.axis_size(axis)
    return lax.ppermute(shard, axis, [(i, (i + by) % size) for i in range(size)])


def swapped(shard, axis, odd):
    size = lax.axis_size(axis)
    assert size % 2 == 0
    ahead = [(i, (i + 1) % size) for i in range(odd, size, 2)]
    return lax.ppermute(shard, axis, ahead + [(j, i) for i, j in ahead])


def rolled(tile, shift, axis):
    shift = shift % tile.shape[axis]
    return pltpu.roll(tile, shift, axis) if shift else tile


class Shifts:
    def __init__(self, rows, depth, width):
        self.rows, self.depth, self.width = (rows, depth, width)
        self.shape = (rows * depth, width)
        sub = lax.broadcasted_iota(jnp.int32, self.shape, 0)
        self.lane = lax.broadcasted_iota(jnp.int32, self.shape, 1)
        self.row = sub // depth
        self.plane = sub % depth
        self.x = self.lane % NX
        self.odd = (self.plane + self.lane // NX + self.x) % 2 == 1

    def select(self, dst):
        return self.odd if dst == 0 else jnp.logical_not(self.odd)

    def t_rows(self, own, other, by):
        if by == 0:
            return own
        near = self.row >= by if by > 0 else self.row < self.rows + by
        return rolled(jnp.where(near, own, other), -by * self.depth, 0)

    def t(self, own, other, by, dst):
        sel = self.select(dst)
        half = {1: (1, 0), 3: (2, 1), -1: (0, -1), -3: (-1, -2)}[by]
        return jnp.where(sel, self.t_rows(own, other, half[0]), self.t_rows(own, other, half[1]))

    def z(self, own, other, by):
        near = self.plane < self.depth - by if by > 0 else self.plane >= -by
        wrap = self.depth - by if by > 0 else -self.depth - by
        return jnp.where(near, rolled(own, -by, 0), rolled(other, wrap, 0))

    def y(self, own, other, by):
        lanes = by * NX
        near = self.lane >= lanes if by > 0 else self.lane < self.width + lanes
        return rolled(jnp.where(near, own, other), -lanes, 1)

    def x_(self, own, by):
        near = self.x < NX - by if by > 0 else self.x >= -by
        wrap = NX - by if by > 0 else -NX - by
        return jnp.where(near, rolled(own, -by, 1), rolled(own, wrap, 1))

    def hop(self, own, other, mu, by, dst):
        if mu == 0:
            return self.t(own, other, by, dst)
        if mu == 1:
            return self.z(own, other, by)
        if mu == 2:
            return self.y(own, other, by)
        return self.x_(own, by)


HOPS = tuple((mu, by) for mu in range(4) for by in (1, 3, -1, -3))


def link_table(fat, long, near, dims, dst):
    rows, depth, width = dims
    tile = (rows * depth, width)

    def body(fat_ref, long_ref, t_ref, z_ref, y_ref, out):
        shifts = Shifts(rows, depth, width)
        lows = (t_ref, z_ref, y_ref)

        def flat(block):
            return block.astype(jnp.float32).reshape(tile)

        def entry(i, carry):
            flip = 3 * (i % 3) + i // 3
            for k, (mu, by) in enumerate(HOPS):
                kind = 0 if abs(by) == 1 else 1
                ref = (fat_ref, long_ref)[kind]
                for part in range(2):
                    if by > 0:
                        value = flat(ref[dst, mu, part, i // 3, i % 3])
                        out[18 * k + 9 * part + i] = value
                    else:
                        own = flat(ref[1 - dst, mu, part, i // 3, i % 3])
                        other = own
                        if mu < 3:
                            other = flat(lows[mu][kind, 1 - dst, part, i // 3, i % 3])
                        value = shifts.hop(own, other, mu, by, dst)
                        out[18 * k + 9 * part + flip] = value if part else -value
            return carry

        lax.fori_loop(0, 9, entry, 0)

    return on_core(body, [(18 * len(HOPS),) + tile], fat, long, *near)[0]


def hopping_sum(shifts, field, near, table, dst):
    flags = near[-1]
    total = [None] * 6
    for mu in range(4):
        ahead = behind = [None] * 6
        if mu < 3:
            one, two = (near[2 * mu], near[2 * mu + 1])
            if one is two:
                ahead = behind = [one[c] for c in range(6)]
            else:
                even = flags[mu] > 0.5
                pairs = [(one[c], two[c]) for c in range(6)]
                ahead = [jnp.where(even, u, v) for u, v in pairs]
                behind = [jnp.where(even, v, u) for u, v in pairs]
        for k, (axis, by) in enumerate(HOPS):
            if axis != mu:
                continue
            other = ahead if by > 0 else behind
            hopped = [shifts.hop(field[c], other[c], mu, by, dst) for c in range(6)]
            for a in range(3):
                re = im = None
                for b in range(3):
                    lre = table[18 * k + 3 * a + b]
                    lim = table[18 * k + 9 + 3 * a + b]
                    vre, vim = (hopped[b], hopped[3 + b])
                    x, y = (lre * vre - lim * vim, lre * vim + lim * vre)
                    re = x if re is None else re + x
                    im = y if im is None else im + y
                total[a] = re if total[a] is None else total[a] + re
                total[3 + a] = im if total[3 + a] is None else total[3 + a] + im
    return total


def axis_sizes():
    return tuple(lax.axis_size(axis) for axis in AXES)


def swaps_of(sizes):
    return tuple(
        (mu, odd) for odd in (1, 0) for mu in (2, 0, 1) if odd == 0 or sizes[mu] > 2
    )


def neighbours(field):
    return tuple(swapped(field, AXES[mu], odd) for mu, odd in swaps_of(axis_sizes()))


def spread(refs, sizes):
    keys = swaps_of(sizes)
    got = dict(zip(keys, refs))
    near = [got.get((mu, odd), got[mu, 0]) for mu in range(3) for odd in (0, 1)]
    return near, list(refs[len(keys) :])


def odd_from_even(field, near, table, flags, dims):
    sizes = axis_sizes()

    def body(field_ref, table_ref, flags_ref, *refs):
        others, (out,) = spread(refs, sizes)
        shifts = Shifts(*dims)
        terms = hopping_sum(shifts, field_ref, others + [flags_ref], table_ref, 1)
        for c, value in enumerate(terms):
            out[c] = value

    return on_core(body, [field.shape], field, table, flags, *near)[0]


def even_from_odd(field, near, start, table, flags, dims, finish, *extra):
    sizes = axis_sizes()

    def body(field_ref, start_ref, table_ref, flags_ref, *refs):
        others, rest = spread(refs, sizes)
        more, out = (rest[:-1], rest[-1])
        shifts = Shifts(*dims)
        terms = hopping_sum(shifts, field_ref, others + [flags_ref], table_ref, 0)
        for c, value in enumerate(terms):
            out[c] = finish(value, start_ref[c], c, more)

    return on_core(body, [field.shape], field, start, table, flags, *near, *extra)[0]


def pairs_of(count):
    return tuple((i, j) for i in range(count) for j in range(i, count)) + ((count, count),)


def gram_parts(basis, odd, copies):
    fields = tuple(basis) + (odd,)
    parts, width = odd.shape[0], 128

    def body(*refs):
        out = refs[-1]
        lane = lax.broadcasted_iota(jnp.int32, (1, width), 1)
        packed = jnp.zeros((1, width), jnp.float32)
        for n, (i, j) in enumerate(pairs_of(len(basis))):
            tile = refs[i][0] * refs[j][0]
            for c in range(1, parts):
                tile = tile + refs[i][c] * refs[j][c]
            value = jnp.sum(jnp.sum(tile, axis=0, keepdims=True), axis=1, keepdims=True)
            packed = jnp.where(lane == n, value, packed)
        for k in range(copies):
            out[k] = packed

    return on_core(body, [(copies, 1, width)], *fields)[0]


def add(a, b):
    return b if a is None else a if b is None else a + b


def times(s, vec):
    return {i: s * v for i, v in vec.items()}


def plus(u, v):
    return {i: add(u.get(i), v.get(i)) for i in sorted(set(u) | set(v))}


def iterations(count, gram, applied, residual, direction, norm, gain):
    def dot(u, v):
        out = None
        for i, a in u.items():
            part = None
            for j, b in v.items():
                part = add(part, gram[i, j] * b)
            out = add(out, a * part)
        return out

    log = []
    for step in range(count):
        image = applied(direction)
        alpha = norm / dot(direction, image)
        gain = plus(gain, times(alpha, direction))
        residual = plus(residual, times(-alpha, image))
        last = direction
        if step + 1 < count:
            norm_next = dot(residual, residual)
            log.append((alpha, norm_next / norm, norm))
            direction = plus(residual, times(norm_next / norm, direction))
            norm = norm_next
        else:
            log.append((alpha, None, norm))
    return gain, residual, last, log


def gram_of(sums_ref, count, tile, applied):
    total = sums_ref[0]
    for k in range(1, sums_ref.shape[0]):
        total = total + sums_ref[k]
    gram = {}
    for n, (i, j) in enumerate(pairs_of(count)):
        value = jnp.broadcast_to(total[:, n : n + 1], tile)
        gram[i, j] = gram[j, i] = value
    last = count - 1
    square = gram.pop((count, count))
    one = jnp.ones(tile, jnp.float32)
    image = applied({last: one})
    top = image.pop(count)
    for i in range(count):
        if i < last:
            product = sum(b * gram[k, last] for k, b in applied({i: one}).items())
        else:
            product = mass_squared * gram[last, last] + square
        for k, b in image.items():
            product = product - b * gram[i, k]
        gram[i, count] = gram[count, i] = product / top
    return gram


def first_update(sums, basis):
    shape = basis[0].shape
    tile = shape[1:]

    def body(sums_ref, v0, v1, v2, state_out, r_out):
        def applied(u):
            return {i + 1: a * (1.0 / SCALE) for i, a in u.items()}

        gram = gram_of(sums_ref, FIRST, tile, applied)
        start = {0: jnp.ones(tile, jnp.float32)}
        gain, residual, direction, log = iterations(
            FIRST, gram, applied, start, start, gram[0, 0], {}
        )
        (alpha0, beta0, _), (alpha1, _, norm) = log
        centre = 1.0 / alpha1 + beta0 / alpha0
        width = jnp.maximum(jnp.sqrt(jnp.maximum(beta0, 0.0)) / alpha0, 1e-3 * centre)
        kept = (
            norm, direction[0], direction[1], gain[0], gain[1],
            residual[0], residual[1], residual[2], centre, width, 1.0 / width,
        )
        for n, value in enumerate(kept):
            state_out[n] = value
        for c in range(shape[0]):
            r_out[c] = residual[0] * v0[c] + residual[1] * v1[c] + residual[2] * v2[c]

    return on_core(body, [(STATE,) + tile, shape], sums, *basis)


STATE = 11
CENTRE, INVERSE = (8, 10)


def last_update(sums, state, basis):
    shape = basis[0].shape
    tile = shape[1:]
    count = len(basis) - 1

    def body(sums_ref, state_ref, *refs):
        vectors, (x_out, true_out) = (refs[:-2], refs[-2:])
        kept = [state_ref[n] for n in range(STATE)]
        norm_before, p0, p1, g0, g1, c0, c1, c2, centre, width, _ = kept
        share = (1.0 / SCALE) / c2
        second = {0: -share * c0, 1: -share * c1, 2: share}

        def applied(u):
            out = {}
            for i, a in u.items():
                if i == 0:
                    out = plus(out, {1: a * (1.0 / SCALE)})
                elif i == 1:
                    out = plus(out, times(a, second))
                else:
                    wide = a * width
                    out = plus(out, {i: a * centre, i + 1: wide})
                    if i > 2:
                        out = plus(out, {i - 1: wide})
            return out

        gram = gram_of(sums_ref, count, tile, applied)
        one = jnp.ones(tile, jnp.float32)
        norm = gram[2, 2]
        ratio = norm / norm_before
        direction = {0: ratio * p0, 1: ratio * p1, 2: one}
        gain, _, _, _ = iterations(
            ITERS - FIRST, gram, applied, {2: one}, direction, norm, {0: g0, 1: g1}
        )
        shown = applied(gain)
        for c in range(shape[0]):
            values = [vector[c] for vector in vectors]
            x_out[c] = sum(s * values[i] for i, s in gain.items())
            true_out[c] = values[0] - sum(s * values[i] for i, s in shown.items())

    return on_core(body, [shape] * 2, sums, state, *basis)


def per_device(source, fat_links, long_links):
    rows, depth, width = source.shape[2:]
    dims = (rows, depth, width)
    tile = (rows * depth, width)
    field = source.reshape((6,) + tile)
    fat, long = (fat_links, long_links)
    near = {
        mu: passed_along(jnp.stack([fat[:, mu], long[:, mu]]), AXES[mu], 1) for mu in (2, 0, 1)
    }
    near = [near[mu] for mu in range(3)]
    odd_table = link_table(fat, long, near, dims, 1)
    even_table = link_table(fat, long, near, dims, 0)
    even = jnp.stack([lax.axis_index(axis) % 2 == 0 for axis in AXES])
    flags = jnp.broadcast_to(even.astype(jnp.float32)[:, None, None], (len(AXES),) + tile)

    devices = 1
    for size in axis_sizes():
        devices *= size

    def half(vector):
        return odd_from_even(vector, neighbours(vector), odd_table, flags, dims)

    def image(vector, odd, near, finish, *extra):
        return even_from_odd(odd, near, vector, even_table, flags, dims, finish, *extra)

    def summed(basis, odd):
        return lax.all_to_all(gram_parts(basis, odd, devices), AXES, 0, 0, tiled=True)

    def scaled(value, vector, c, more):
        return SCALE * (mass_squared * vector - value)

    def shifted(value, vector, c, more):
        state = more[0]
        value = ((mass_squared - state[CENTRE]) * vector - value) * state[INVERSE]
        return value - more[1][c] if len(more) > 1 else value

    def summed_beside(basis, odd, finish, *extra):
        near = neighbours(odd)
        sums = summed(basis, odd)
        return sums, image(basis[-1], odd, near, finish, *extra)

    basis, odd = ([field], half(field))
    for _ in range(FIRST - 1):
        basis.append(image(basis[-1], odd, neighbours(odd), scaled))
        odd = half(basis[-1])
    sums, last = summed_beside(basis, odd, scaled)
    state, residual = first_update(sums, basis + [last])
    basis.append(residual)
    odd = half(residual)
    extra = (state,)
    for _ in range(ITERS - FIRST - 1):
        basis.append(image(basis[-1], odd, neighbours(odd), shifted, *extra))
        extra = (state, basis[-2])
        odd = half(basis[-1])
    sums, last = summed_beside(basis, odd, shifted, *extra)
    solution, true = last_update(sums, state, basis + [last])
    return (solution.reshape(source.shape), true.reshape(source.shape))


def solution(mesh):
    in_specs = (
        P(None, None, "ta", "gz", "gy"),
        P(None, None, None, None, None, "ta", "gz", "gy"),
        P(None, None, None, None, None, "ta", "gz", "gy"),
    )
    out_specs = (P(None, None, "ta", "gz", "gy"), P(None, None, "ta", "gz", "gy"))
    return jax.shard_map(
        per_device, mesh=mesh, in_specs=in_specs, out_specs=out_specs, check_vma=False
    )
```
